32 devices in a mesh: ctx: 16 (over z, x, core), head: 2 (over y).
Axes of the slice: x: 2, y: 2, z: 4, core: 2. Of those that a mesh axis runs over, the one named last changes fastest.
Arguments:
- queries: bfloat16 [4096, 32, 128], P('ctx', 'head'), may hold values from -300 to 300
- key_rows: bfloat16 [4096, 4, 128], P('ctx', 'head'), may hold values from -6 to 6
- value_vectors: bfloat16 [4096, 4, 128], P('ctx', 'head'), may hold values from -6 to 6
- doc_ids: int32 [4096], replicated, may hold values from 0 to 2, never falling along the last dimension, each value on 1 to 1792 neighbouring positions
Outputs:
- attended: bfloat16 [4096, 32, 128], P(('ctx', 'head'))
The draws below stay inside these ranges and needn't reach their ends.
Inputs may be any that keep to these rules, and one draw needn't show every extreme that they name: `doc_ids`: ids never fall along the pack and each prompt holds at most 1792 tokens.
All inputs are finite; a program needn't handle non-finite values.
Results may differ from the reference program's by a relative error of at most 0.008.
Values may be sent and summed in bfloat16 or wider, within the bound.
No kernel may reach another device: no remote copies, remote signals or barrier semaphores. Data moves between devices by JAX's collectives and lax.ppermute only.
A program may use at most 64 MiB of HBM per device.

```python
import math
import jax
import jax.numpy as jnp
import numpy as np
from jax import lax

QUERY_HEADS = 32
KEY_VALUE_HEADS = 4
HEAD_SIZE = 128
TOKENS_PER_SHARD = 256
PROMPTS = 3
REACH = 7
PACKED_TOKENS = 4096
N_CTX = 16


def drawn_pair(key):
    key_sample = jax.random.fold_in(key, 11)
    query_draw = jax.random.fold_in(key, 23)
    key_entries = jnp.clip(jax.random.normal(key_sample, (PACKED_TOKENS, KEY_VALUE_HEADS, HEAD_SIZE), jnp.float32), -6.0, 6.0)
    query_vals = jnp.clip(jax.random.normal(query_draw, (PACKED_TOKENS, QUERY_HEADS, HEAD_SIZE), jnp.float32), -6.0, 6.0)
    return (query_vals, key_entries)


def draw_queries(key, part):
    return drawn_pair(key)[0].astype(jnp.bfloat16)


def draw_key_rows(key, part):
    return drawn_pair(key)[1].astype(jnp.bfloat16)


def steps_of(stream_key, dims, shards, smallest, largest):
    loudness = 1.0
    for dim, parts in shards:
        draws = jax.random.uniform(jax.random.fold_in(jax.random.fold_in(stream_key, 6), dim), (parts,), jnp.float32, smallest / len(shards), largest / len(shards))
        loudness = loudness * jnp.repeat(jnp.exp(draws), dims[dim] // parts).reshape((-1,) + (1,) * (len(dims) - 1 - dim))
    return loudness


def split_up(count, total, reach, lean):
    weights = [(1 << 20) // math.isqrt(rank ** lean) + 1 for rank in range(2, count + 1)]
    spare, given = total - reach - (count - 1), [1] * (count - 1)
    while spare > 0:
        candidates = [i for i in range(count - 1) if given[i] < reach]
        pool, left = sum([weights[i] for i in candidates]), spare
        for i in candidates:
            more = min(reach - given[i], max(1, left * weights[i] // pool), spare)
            given[i] = given[i] + more
            spare = spare - more
    return np.array([reach] + given)


def uneven(stream_key, count, total, limit, skew):
    if count == 2:
        one = jax.random.randint(stream_key, (), max(1, total - limit), min(limit, total - 1) + 1)
        return jnp.stack([one, total - one])
    lengths = jnp.asarray(split_up(count, total, limit, skew), jnp.int32)
    twos = (count - 1) // 2
    giver, taker = lengths[1:1 + 2 * twos:2], lengths[2:2 + 2 * twos:2]
    margin = jnp.minimum(giver - 1, limit - taker)
    shifted = jax.random.randint(jax.random.fold_in(stream_key, 1), (twos,), 0, 1 << 20) % (margin + 1)
    lengths = lengths.at[1:1 + 2 * twos:2].set(giver - shifted).at[2:2 + 2 * twos:2].set(taker + shifted)
    return lengths[jax.random.permutation(jax.random.fold_in(stream_key, 2), count)]


def noise(own_key, dims, scale, most, cuts=(), kind=jnp.bfloat16):
    loudness = steps_of(own_key, dims, cuts, -0.22, 0.18) if cuts else 1.0
    result = jax.random.normal(own_key, dims, jnp.float32) * scale * loudness
    return jnp.minimum(jnp.maximum(result, -most), most).astype(kind)


def setup_inputs(seed: int = 0) -> dict:
    key_of = jax.random.split(jax.random.key(seed), 5)
    return {
        "queries": draw_queries(jax.random.fold_in(key_of[4], 71), 0),
        "key_rows": draw_key_rows(jax.random.fold_in(key_of[4], 71), 0),
        "value_vectors": noise(key_of[2], (PACKED_TOKENS, KEY_VALUE_HEADS, HEAD_SIZE), 1.0, 6.0, ((0, 16), (1, 2))),
        "doc_ids": jnp.searchsorted(jnp.cumsum(uneven(key_of[3], PROMPTS, PACKED_TOKENS, REACH * TOKENS_PER_SHARD, 2)), jnp.arange(PACKED_TOKENS), side="right").astype(jnp.int32),
    }


def reference(queries, key_rows, value_vectors, doc_ids):
    head_group = QUERY_HEADS // KEY_VALUE_HEADS
    window = (REACH + 1) * TOKENS_PER_SHARD
    inv_root = HEAD_SIZE ** -0.5

    def query_block(block_num):
        query_offset = (block_num * TOKENS_PER_SHARD).astype(jnp.int32)
        k_start = jnp.maximum(query_offset - REACH * TOKENS_PER_SHARD, 0).astype(jnp.int32)
        query_portion = lax.dynamic_slice_in_dim(queries, query_offset, TOKENS_PER_SHARD, 0).reshape(TOKENS_PER_SHARD, KEY_VALUE_HEADS, head_group, HEAD_SIZE).astype(jnp.float32)
        k_part = lax.dynamic_slice_in_dim(key_rows, k_start, window, 0).astype(jnp.float32)
        v_part = lax.dynamic_slice_in_dim(value_vectors, k_start, window, 0).astype(jnp.float32)
        q_doc = lax.dynamic_slice_in_dim(doc_ids, query_offset, TOKENS_PER_SHARD, 0)
        k_doc = lax.dynamic_slice_in_dim(doc_ids, k_start, window, 0)
        q_pos = query_offset + jnp.arange(TOKENS_PER_SHARD, dtype=jnp.int32)
        k_pos = k_start + jnp.arange(window, dtype=jnp.int32)
        visible = (q_doc[:, None] == k_doc[None, :]) & (k_pos[None, :] <= q_pos[:, None])
        scores = jnp.einsum('tgrd,ugd->grtu', query_portion, k_part) * inv_root
        masked = jnp.where(visible, scores, -jnp.inf)
        row_max = jnp.max(masked, axis=-1, keepdims=True)
        weights = jnp.where(visible, jnp.exp(scores - row_max), 0.0)
        total = jnp.sum(weights, axis=-1, keepdims=True)
        rounded = lax.optimization_barrier(weights.astype(jnp.bfloat16)).astype(jnp.float32)
        summed = jnp.einsum('grtu,ugd->grtd', rounded, v_part) / total
        return summed.transpose(2, 0, 1, 3).reshape(TOKENS_PER_SHARD, QUERY_HEADS, HEAD_SIZE).astype(jnp.bfloat16)

    blocks = lax.map(query_block, jnp.arange(N_CTX, dtype=jnp.int32))
    return blocks.reshape(PACKED_TOKENS, QUERY_HEADS, HEAD_SIZE)
```

```python
import functools
import math

import jax
import jax.numpy as jnp
from jax import lax
from jax.experimental import pallas as pl
from jax.experimental.pallas import tpu as pltpu
from jax.sharding import PartitionSpec as P


QUAD = 4
TILE_TOKENS = 32
HIDDEN = -1e30


def shifted(block, distance):
    n = lax.axis_size("ctx")
    return lax.ppermute(block, "ctx", [(i, (i + distance) % n) for i in range(n)])


def swapped(block, bit):
    n = lax.axis_size("ctx")
    return lax.ppermute(block, "ctx", [(i, i ^ bit) for i in range(n)])


def pack_kernel(k_ref, v_ref, *outs):
    tok = k_ref.shape[0]
    for g, out in enumerate(outs):
        out[0:tok, :] = k_ref[:, g, :]
        v = v_ref[:, g, :].astype(jnp.float32)
        out[tok : 2 * tok, :] = jnp.concatenate(
            [v[h : h + 128, :].T for h in range(0, tok, 128)], axis=0
        ).astype(jnp.bfloat16)


def packed(key_rows, value_vectors):
    tok, kv_heads, dim = key_rows.shape
    return pl.pallas_call(
        pack_kernel,
        out_shape=[jax.ShapeDtypeStruct((2 * tok, dim), jnp.bfloat16)] * kv_heads,
        name="pack",
    )(key_rows, value_vectors)


def attend_kernel(hops, scale, meta_ref, start_ref, q_ref, *refs):
    n_slots = 4 * hops + 1
    slots = refs[:n_slots]
    out_ref = refs[n_slots]
    kbuf, acc_ref, max_ref, sum_ref, sem = refs[n_slots + 1 :]
    tok, group, dim = q_ref.shape
    rows = TILE_TOKENS * group
    tiles = tok // TILE_TOKENS
    me, first_start, last_start = meta_ref[0], meta_ref[1], meta_ref[2]
    last_hop = jnp.where((me >> 1) & 1, 0, hops)

    def block_of(s):
        hop = jnp.where(s < 2, 0, (s + 2) >> 2)
        hop = jnp.where(s >= n_slots - 3, hops, hop)
        turn = jnp.where(s < 2, s, (s + 2) & 3)
        turn = jnp.where(s >= n_slots - 3, s - (n_slots - 4), turn)
        hop = jnp.where(s >= n_slots - 2, last_hop, hop)
        return (me ^ turn) - QUAD * hop

    def mode_of(s):
        block = block_of(s)
        low = block * tok
        live = (block >= 0) & (block < me) & (low + tok > first_start)
        return low, live, low >= last_start

    def fetch(s):
        return pltpu.make_async_copy(slots[s], kbuf.at[s], sem.at[s])

    fetch(0).start()
    for s in range(1, n_slots):
        pl.when(mode_of(s)[1])(lambda s=s: fetch(s).start())
    fetch(0).wait()

    def tile(s, r, count, low, masked, first):
        keys = kbuf[s, 0:count, :]
        values = jnp.concatenate(
            [kbuf[s, pl.ds(tok + h, 128), :] for h in range(0, count, 128)], axis=1
        )
        q = q_ref[r * TILE_TOKENS : (r + 1) * TILE_TOKENS].reshape(rows, dim)
        scores = lax.dot_general(
            keys, q, (((1,), (1,)), ((), ())), preferred_element_type=jnp.float32
        )
        if masked:
            key_pos = low + lax.broadcasted_iota(jnp.int32, (count, rows), 0)
            seen = key_pos >= start_ref[r : r + 1, :]
            if first:
                lane = lax.broadcasted_iota(jnp.int32, (count, rows), 1)
                seen = seen & (key_pos <= me * tok + r * TILE_TOKENS + lane // group)
            scores = jnp.where(seen, scores, HIDDEN)
        top = jnp.max(scores, axis=0, keepdims=True) * scale
        if not first:
            old = max_ref[r : r + 1, :]
            top = jnp.maximum(old, top)
        weights = jnp.exp2(scores * scale - top)
        total = jnp.sum(weights, axis=0, keepdims=True)
        product = lax.dot_general(
            values,
            weights.astype(jnp.bfloat16),
            (((1,), (0,)), ((), ())),
            preferred_element_type=jnp.float32,
        )
        if not first:
            fade = jnp.exp2(old - top)
            total = total + sum_ref[r : r + 1, :] * fade
            product = product + acc_ref[r] * fade
        max_ref[r : r + 1, :] = top
        sum_ref[r : r + 1, :] = total
        acc_ref[r] = product

    for r in range(tiles):
        count = -(-((r + 1) * TILE_TOKENS) // 128) * 128
        tile(0, r, count, me * tok, True, True)

    def visit(s, carry):
        low, live, whole = mode_of(s)

        @pl.when(live)
        def _():
            pltpu.make_async_copy(slots[0], kbuf.at[s], sem.at[s]).wait()

            @pl.when(whole)
            def _():
                for r in range(tiles):
                    tile(s, r, tok, low, False, False)

            @pl.when(jnp.logical_not(whole))
            def _():
                for r in range(tiles):
                    tile(s, r, tok, low, True, False)

        return carry

    lax.fori_loop(1, n_slots, visit, 0)
    for r in range(tiles):
        done = acc_ref[r] * pl.reciprocal(sum_ref[r : r + 1, :], approx=False)
        out_ref[r * TILE_TOKENS : (r + 1) * TILE_TOKENS] = (
            done.T.reshape(TILE_TOKENS, group, dim).astype(jnp.bfloat16)
        )


def attended(hops, g, group, meta, starts, queries, slots):
    tok, heads, dim = queries.shape
    n_slots = len(slots)
    rows = TILE_TOKENS * group
    tiles = tok // TILE_TOKENS
    scale = dim ** (-0.5) * math.log2(math.e)
    return pl.pallas_call(
        functools.partial(attend_kernel, hops, scale),
        out_shape=jax.ShapeDtypeStruct((tok, group, dim), jnp.bfloat16),
        grid=(1,),
        in_specs=[
            pl.BlockSpec(memory_space=pltpu.SMEM),
            pl.BlockSpec((tiles, rows), lambda i: (0, 0)),
            pl.BlockSpec((tok, group, dim), lambda i: (0, g, 0)),
        ]
        + [pl.BlockSpec(memory_space=pl.ANY)] * n_slots,
        out_specs=pl.BlockSpec((tok, group, dim), lambda i: (0, 0, 0)),
        scratch_shapes=[
            pltpu.VMEM((n_slots, 2 * tok, dim), jnp.bfloat16),
            pltpu.VMEM((tiles, dim, rows), jnp.float32),
            pltpu.VMEM((tiles, rows), jnp.float32),
            pltpu.VMEM((tiles, rows), jnp.float32),
            pltpu.SemaphoreType.DMA((n_slots,)),
        ],
        name="attend",
    )(meta, starts, queries, *slots)


def body(queries, key_rows, value_vectors, doc_ids):
    tok, heads_here, dim = queries.shape
    kv_heads = key_rows.shape[1]
    group = heads_here // kv_heads
    cycle = lax.axis_size("ctx")
    reach = cycle // 2 - 1
    hops = -(-reach // QUAD)
    me = lax.axis_index("ctx")
    own_doc = lax.dynamic_slice_in_dim(doc_ids, me * tok, tok, 0)
    own_start = jnp.sum((doc_ids[None, :] < own_doc[:, None]).astype(jnp.int32), axis=1)
    starts = jnp.repeat(own_start, group).reshape(tok // TILE_TOKENS, TILE_TOKENS * group)
    meta = jnp.stack([me.astype(jnp.int32), own_start[0], own_start[-1]])
    left_column = (me >> 1) & 1 == 0

    own = packed(key_rows, value_vectors)
    outs = []
    for g in range(kv_heads):
        line = own[g]
        slots = [line, swapped(line, 1)]
        for hop in range(1, hops + 1):
            line = shifted(line, QUAD)
            if hop < hops:
                across = swapped(line, 2)
                slots += [line, swapped(line, 1), across, swapped(across, 1)]
        slots.append(swapped(line, 1))
        across = swapped(jnp.where(left_column, own[g], line), 2)
        slots += [across, swapped(across, 1)]
        outs.append(attended(hops, g, group, meta, starts, queries, slots))

    half = tok // 2
    side = lax.axis_index("head")
    pieces = []
    for out in outs:
        away = lax.dynamic_slice_in_dim(out, (1 - side) * half, half, 0)
        home = lax.dynamic_slice_in_dim(out, side * half, half, 0)
        other = lax.ppermute(away, "head", [(0, 1), (1, 0)])
        pieces.append((home, other))
    mine = jnp.concatenate([p[0] for p in pieces], axis=1)
    theirs = jnp.concatenate([p[1] for p in pieces], axis=1)
    low = jnp.where(side == 0, mine, theirs)
    high = jnp.where(side == 0, theirs, mine)
    return jnp.concatenate([low, high], axis=1)


def solution(mesh):
    placed = (P("ctx", "head", None), P("ctx", "head", None), P("ctx", "head", None), P())
    return jax.shard_map(
        body, mesh=mesh, in_specs=placed, out_specs=P(("ctx", "head"), None, None), check_vma=False
    )
```

```python
import functools
import math

import jax
import jax.numpy as jnp
from jax import lax
from jax.experimental import pallas as pl
from jax.experimental.pallas import tpu as pltpu
from jax.sharding import PartitionSpec as P


QUAD = 4
CHUNK = 512
NEAR_HOPS = 3
HIDDEN = -1e30
CEILING = 2.0**100
FLOOR = 2.0**-100


def shifted(block, distance):
    n = lax.axis_size("ctx")
    return lax.ppermute(block, "ctx", [(i, (i + distance) % n) for i in range(n)])


def swapped(block, bit):
    n = lax.axis_size("ctx")
    return lax.ppermute(block, "ctx", [(i, i ^ bit) for i in range(n)])


def in_vmem(count):
    return [pl.BlockSpec(memory_space=pltpu.VMEM)] * count


def hops_needed():
    reach = lax.axis_size("ctx") // 2 - 1
    return -(-reach // QUAD)


def near(*arrays):
    if hops_needed() > NEAR_HOPS:
        return list(arrays)
    return [pltpu.with_memory_space_constraint(a, pltpu.VMEM) for a in arrays]


def near_shape(shape, dtype):
    if hops_needed() > NEAR_HOPS:
        return jax.ShapeDtypeStruct(shape, dtype)
    return pltpu.VMEM(shape, dtype)


def pack_kernel(k_ref, v_ref, *refs):
    *outs, k_wide, v_wide = refs
    heads = len(outs)
    tok = k_ref.shape[0] // heads
    k_wide[...] = k_ref[...].astype(jnp.float32)
    v_wide[...] = v_ref[...].astype(jnp.float32)
    for g, out in enumerate(outs):
        out[0:tok, :] = k_wide[pl.ds(g, tok, heads), :].astype(jnp.bfloat16)
        out[tok : 2 * tok, :] = v_wide[pl.ds(g, tok, heads), :].astype(jnp.bfloat16)


def packed(key_rows, value_vectors):
    tok, kv_heads, dim = key_rows.shape
    flat = (tok * kv_heads, dim)
    return pl.pallas_call(
        pack_kernel,
        out_shape=[near_shape((2 * tok, dim), jnp.bfloat16)] * kv_heads,
        in_specs=in_vmem(2),
        out_specs=in_vmem(kv_heads),
        scratch_shapes=[pltpu.VMEM(flat, jnp.float32)] * 2,
        name="pack",
    )(key_rows.reshape(flat), value_vectors.reshape(flat))


def join_kernel(choose, *refs):
    *ins, out_ref = refs
    size = ins[0].shape[0]
    if choose:
        odd = lax.axis_index("ctx") & 1
        own, line, across = ins

        @pl.when(odd == 1)
        def _():
            out_ref[0:size, :] = line[...]

        @pl.when(odd == 0)
        def _():
            out_ref[0:size, :] = own[...]

        out_ref[size:, :] = across[...]
    else:
        out_ref[0:size, :] = ins[0][...]
        out_ref[size:, :] = ins[1][...]


def joined(*arrays):
    size, dim = arrays[0].shape
    return pl.pallas_call(
        functools.partial(join_kernel, len(arrays) == 3),
        out_shape=near_shape((2 * size, dim), jnp.bfloat16),
        in_specs=in_vmem(len(arrays)),
        out_specs=pl.BlockSpec(memory_space=pltpu.VMEM),
        name="join",
    )(*near(*arrays))


def attend_kernel(hops, scale, n_early, early, late, docs_ref, q_ref, *refs):
    refs = list(refs)
    n_arrays = (1 + 2 * (hops - 1) + 2) if late else n_early
    arrays = [refs.pop(0) for _ in range(n_arrays)]
    state_in = refs.pop(0) if late and not early else None
    outs = [refs.pop(0) for _ in range(2 if late else 1)]
    kbuf, acc_ref, p_buf, low_ref = refs[:4]
    top_ref = refs[4] if late else None
    tok, group, dim = q_ref.shape
    chunks = tok * group // CHUNK
    span = tok // chunks
    me = lax.axis_index("ctx")
    side = lax.axis_index("head")
    docs = docs_ref[...]
    bound_1 = jnp.sum((docs < 1).astype(jnp.int32))
    bound_2 = jnp.sum((docs < 2).astype(jnp.int32))

    def start_of(pos):
        return jnp.where(pos >= bound_2, bound_2, jnp.where(pos >= bound_1, bound_1, 0))

    first_start = start_of(me * tok)
    last_start = start_of(me * tok + tok - 1)
    right = (me >> 1) & 1
    far = jnp.where(right == 1, 0, hops)
    table = [(0, 0, 0, 0)]
    for hop in range(1, hops):
        a = 2 * hop - 1
        table += [(a, 0, 0, hop), (a, 1, 2, hop), (a + 1, 0, 1, hop), (a + 1, 1, 3, hop)]
    n_near = len(table)
    a = 2 * hops - 1
    table += [(a, 1, 2, far), (a + 1, 0, 1, jnp.where(me & 1 == 1, 0, hops)), (a + 1, 1, 3, far)]
    n_slots = len(table)

    def load(s):
        array, part, turn, hop = table[s]
        block = (me ^ turn) - QUAD * hop
        low = block * tok
        live = (block >= 0) & (block < me) & (low + tok > first_start)
        if s == 0:
            live = block == me
        low_ref[s] = jnp.where(live, low, -1)

        @pl.when(live)
        def _():
            kbuf[s] = arrays[array][2 * tok * part : 2 * tok * (part + 1), :]

    def queries_of(r):
        return q_ref[r * span : (r + 1) * span].reshape(CHUNK, dim)

    def scores_of(s, q):
        return lax.dot_general(
            q, kbuf[s, 0:tok, :], (((1,), (1,)), ((), ())), preferred_element_type=jnp.float32
        )

    def visible(r, low):
        row = lax.broadcasted_iota(jnp.int32, (CHUNK, tok), 0)
        key = lax.broadcasted_iota(jnp.int32, (CHUNK, tok), 1) + low
        pos = row // group + (me * tok + r * span)
        return (key >= start_of(pos)) & (key <= pos)

    def values_of(s):
        ones = jnp.ones((tok, dim), jnp.bfloat16)
        return jnp.concatenate([kbuf[s, tok : 2 * tok, :], ones], axis=1)

    def product(weights, values):
        return lax.dot_general(
            weights, values, (((1,), (0,)), ((), ())), preferred_element_type=jnp.float32
        )

    def stream_pass(s, low, masked, fresh):
        def weigh(r):
            weights = jnp.exp2(scores_of(s, queries_of(r)) * scale)
            if masked:
                weights = jnp.where(visible(r, low), weights, 0.0)
            p_buf[r % 2] = weights.astype(jnp.bfloat16)

        values = values_of(s)
        weigh(0)
        for r in range(chunks):
            if r + 1 < chunks:
                weigh(r + 1)
            gained = product(p_buf[r % 2], values)
            acc_ref[r] = gained if fresh else acc_ref[r] + gained

    def visit(s, carry):
        low = low_ref[s]
        whole = low >= last_start
        pl.when((low >= 0) & whole)(lambda: stream_pass(s, low, False, False))
        pl.when((low >= 0) & jnp.logical_not(whole))(lambda: stream_pass(s, low, True, False))
        return carry

    if early:
        for s in range(n_near):
            load(s)
        stream_pass(0, me * tok, True, True)
        lax.fori_loop(1, n_near, visit, 0)
    else:
        acc_ref[...] = state_in[...]
    if not late:
        outs[0][...] = acc_ref[...]
        return
    for s in range(n_near, n_slots):
        load(s)
    lax.fori_loop(n_near, n_slots, visit, 0)

    total = acc_ref[:, :, dim:]
    bad = jnp.max(jnp.where((total < CEILING) & (total > FLOOR), 0.0, 1.0))

    @pl.when(bad > 0.0)
    def _():
        if not early:
            for s in range(n_near):
                load(s)
        top_ref[...] = jnp.full_like(top_ref, HIDDEN)
        acc_ref[...] = jnp.zeros_like(acc_ref)

        def careful(i, carry):
            s, r = i // chunks, lax.rem(i, chunks)
            low = low_ref[s]

            @pl.when(low >= 0)
            def _():
                q = q_ref[pl.ds(r * span, span)].reshape(CHUNK, dim)
                scores = jnp.where(visible(r, low), scores_of(s, q) * scale, HIDDEN)
                old = top_ref[r]
                top = jnp.maximum(old, jnp.max(scores, axis=1, keepdims=True))
                weights = jnp.exp2(scores - top[:, 0:1]).astype(jnp.bfloat16)
                fade = jnp.exp2(old - top)
                fade = jnp.concatenate([fade, fade], axis=1)
                acc_ref[r] = acc_ref[r] * fade + product(weights, values_of(s))
                top_ref[r] = top

            return carry

        lax.fori_loop(0, n_slots * chunks, careful, 0)

    half = chunks // 2
    for ref, at in zip(outs, (1 - side, side)):
        for r in range(half):
            both = acc_ref[at * half + r]
            done = both[:, :dim] * pl.reciprocal(both[:, dim:], approx=False)
            ref[r * span : (r + 1) * span] = done.reshape(span, group, dim).astype(jnp.bfloat16)


def attend(hops, g, group, docs, queries, arrays, state, early, late):
    tok, heads, dim = queries.shape
    chunks = tok * group // CHUNK
    scale = dim ** (-0.5) * math.log2(math.e)
    n_slots = 4 * hops
    carried = (chunks, CHUNK, 2 * dim)
    piece = near_shape((tok // 2, group, dim), jnp.bfloat16)
    scratch = [
        pltpu.VMEM((n_slots, 2 * tok, dim), jnp.bfloat16),
        pltpu.VMEM(carried, jnp.float32),
        pltpu.VMEM((2, CHUNK, tok), jnp.bfloat16),
        pltpu.SMEM((n_slots,), jnp.int32),
    ]
    if late:
        scratch.append(pltpu.VMEM((chunks, CHUNK, dim), jnp.float32))
    states = near(state) if late and not early else []
    return pl.pallas_call(
        functools.partial(attend_kernel, hops, scale, len(arrays), early, late),
        out_shape=[piece, piece] if late else [near_shape(carried, jnp.float32)],
        grid=(1,),
        in_specs=[
            pl.BlockSpec(memory_space=pltpu.VMEM),
            pl.BlockSpec((tok, group, dim), lambda i: (0, g, 0)),
        ]
        + in_vmem(len(arrays) + len(states)),
        out_specs=in_vmem(2 if late else 1),
        scratch_shapes=scratch,
        name="attend" if early and late else "early" if early else "late",
    )(docs, queries, *near(*arrays), *states)


def merge_kernel(group, *refs):
    *pieces, out_ref = refs
    heads = out_ref.shape[1]
    side = lax.axis_index("head")
    for g in range(len(pieces) // 2):
        for ref, at in ((pieces[2 * g], side), (pieces[2 * g + 1], 1 - side)):
            first = pl.multiple_of(at * (heads // 2) + g * group, group)
            out_ref[:, pl.ds(first, group), :] = ref[...]


def merged(pieces):
    tok, group, dim = pieces[0].shape
    return pl.pallas_call(
        functools.partial(merge_kernel, group),
        out_shape=jax.ShapeDtypeStruct((tok, group * len(pieces), dim), jnp.bfloat16),
        in_specs=in_vmem(len(pieces)),
        out_specs=pl.BlockSpec(memory_space=pltpu.VMEM),
        name="merge",
    )(*near(*pieces))


SPLIT = False


def body(queries, key_rows, value_vectors, doc_ids):
    tok, heads_here, dim = queries.shape
    kv_heads = key_rows.shape[1]
    group = heads_here // kv_heads
    hops = hops_needed()
    docs = doc_ids.reshape(-1, 128)
    left = (lax.axis_index("ctx") >> 1) & 1 == 0

    own = packed(key_rows, value_vectors)
    pieces = []
    for g in range(kv_heads):
        line = own[g]
        arrays = [line]
        for hop in range(1, hops):
            line = shifted(line, QUAD)
            pair = joined(line, swapped(line, 2))
            arrays += [pair, swapped(pair, 1)]
        n_early = len(arrays)
        line = shifted(line, QUAD)
        across = swapped(jnp.where(left, own[g], line), 2)
        pair = joined(own[g], line, across)
        arrays += [pair, swapped(pair, 1)]
        if SPLIT:
            (state,) = attend(hops, g, group, docs, queries, arrays[:n_early], None, True, False)
            away, home = attend(hops, g, group, docs, queries, arrays, state, False, True)
        else:
            away, home = attend(hops, g, group, docs, queries, arrays, None, True, True)
        pieces += [home, lax.ppermute(away, "head", [(0, 1), (1, 0)])]
    return merged(pieces)


def solution(mesh):
    placed = (P("ctx", "head", None), P("ctx", "head", None), P("ctx", "head", None), P())
    return jax.shard_map(
        body, mesh=mesh, in_specs=placed, out_specs=P(("ctx", "head"), None, None), check_vma=False
    )
```

```python
import functools
import math

import jax
import jax.numpy as jnp
from jax import lax
from jax.experimental import pallas as pl
from jax.experimental.pallas import tpu as pltpu
from jax.sharding import PartitionSpec as P


QUAD = 4
CHUNK = 512
LANES = 128
NEAR_HOPS = 3
HIDDEN = -1e30
FAR_SLOT = 5
EMPTY = -(1 << 30)
SMALL = 64
CEILING = 2.0**100
FLOOR = 2.0**-100


def shifted(block, distance):
    n = lax.axis_size("ctx")
    return lax.ppermute(block, "ctx", [(i, (i + distance) % n) for i in range(n)])


def swapped(block, bit):
    n = lax.axis_size("ctx")
    return lax.ppermute(block, "ctx", [(i, i ^ bit) for i in range(n)])


def crossed(block):
    return lax.ppermute(block, "head", [(0, 1), (1, 0)])


def in_vmem(count):
    return [pl.BlockSpec(memory_space=pltpu.VMEM)] * count


def hops_needed():
    reach = lax.axis_size("ctx") // 2 - 1
    return -(-reach // QUAD)


def near(*arrays):
    if hops_needed() > NEAR_HOPS:
        return list(arrays)
    return [pltpu.with_memory_space_constraint(a, pltpu.VMEM) for a in arrays]


def near_shape(shape, dtype):
    if hops_needed() > NEAR_HOPS:
        return jax.ShapeDtypeStruct(shape, dtype)
    return pltpu.VMEM(shape, dtype)


def pack_kernel(k_ref, v_ref, *refs):
    *outs, k_wide, v_wide = refs
    heads = len(outs)
    tok = k_ref.shape[0] // heads
    k_wide[...] = k_ref[...].astype(jnp.float32)
    v_wide[...] = v_ref[...].astype(jnp.float32)
    for g, out in enumerate(outs):
        out[0:tok, :] = k_wide[pl.ds(g, tok, heads), :].astype(jnp.bfloat16)
        out[tok : 2 * tok, :] = v_wide[pl.ds(g, tok, heads), :].astype(jnp.bfloat16)


def packed(key_rows, value_vectors):
    tok, kv_heads, dim = key_rows.shape
    flat = (tok * kv_heads, dim)
    return pl.pallas_call(
        pack_kernel,
        out_shape=[near_shape((2 * tok, dim), jnp.bfloat16)] * kv_heads,
        in_specs=in_vmem(2),
        out_specs=in_vmem(kv_heads),
        scratch_shapes=[pltpu.VMEM(flat, jnp.float32)] * 2,
        name="pack",
    )(key_rows.reshape(flat), value_vectors.reshape(flat))


def take(out_ref, at, choices):
    for wanted, ref in choices:

        def copy(ref=ref):
            out_ref[at : at + ref.shape[0], :] = ref[...]

        if wanted is None:
            copy()
        else:
            pl.when(wanted)(copy)


def joined(first, second):
    arrays = [array for _, array in first + second]
    size, dim = arrays[0].shape

    def kernel(*refs):
        *ins, out_ref = refs
        me = lax.axis_index("ctx")
        wanted = [None if test is None else test(me) for test, _ in first + second]
        choices = list(zip(wanted, ins))
        take(out_ref, 0, choices[: len(first)])
        take(out_ref, size, choices[len(first) :])

    return pl.pallas_call(
        kernel,
        out_shape=near_shape((2 * size, dim), jnp.bfloat16),
        in_specs=in_vmem(len(arrays)),
        out_specs=pl.BlockSpec(memory_space=pltpu.VMEM),
        name="join",
    )(*near(*arrays))


def upper(me):
    return me & 1 == 1


def lower(me):
    return me & 1 == 0


def right(me):
    return me & 2 == 2


def left(me):
    return me & 2 == 0


def both(test, other):
    return lambda me: test(me) & other(me)


def chosen(test, yes, no):
    return jnp.where(test(lax.axis_index("ctx")), yes, no)


def gathered(own, hops, across_first):
    arrays = [own]
    line = own

    def twin(first, second):
        pair = joined(first, second)
        return [pair, swapped(pair, 1)]

    if across_first:
        beside = swapped(own, 2)
        line = shifted(own, QUAD)
        wide = shifted(chosen(left, beside, line), QUAD)
        back = shifted(line, QUAD)
        arrays += twin([(None, line)], [(right, beside), (left, wide)])
        across = swapped(chosen(left, line, wide), 2)
        last = [(lower, own), (both(upper, right), wide), (both(upper, left), back)]
    else:
        for _ in range(1, hops):
            line = shifted(line, QUAD)
            across = swapped(line, 2)
            arrays += twin([(None, line)], [(None, across)])
        line = shifted(line, QUAD)
        across = swapped(chosen(left, own, line), 2)
        last = [(lower, own), (upper, line)]
    return arrays + [across, twin(last, [(None, across)])[1]]


def slot_table(me, hops, across_first):
    near_hop = jnp.where(right(me), 0, 1)
    far_hop = jnp.where(right(me), 1 if across_first else 0, hops)
    table = [(0, 0, 0, 0)]
    for hop in range(1, hops):
        a = 2 * hop - 1
        beside = near_hop if across_first else hop
        table += [(a, 0, 0, hop), (a, 1, 2, beside)]
        table += [(a + 1, 0, 1, hop), (a + 1, 1, 3, beside)]
    a = 2 * hops - 1
    table += [(a, 0, 2, far_hop), (a + 1, 0, 1, jnp.where(upper(me), 0, hops))]
    return table + [(a + 1, 1, 3, far_hop)]


class Rows:
    def __init__(self, docs_ref, q_ref, group, start_ref, offset, tok):
        self.q_ref, self.group, self.start_ref, self.tok = q_ref, group, start_ref, tok
        count, _, self.dim = q_ref.shape
        self.chunks = count * group // CHUNK
        self.me = lax.axis_index("ctx")
        self.base = self.me * self.tok + offset
        docs = docs_ref[...]
        bound_1 = jnp.sum((docs < 1).astype(jnp.int32))
        bound_2 = jnp.sum((docs < 2).astype(jnp.int32))

        def start_of(pos):
            return jnp.where(pos >= bound_2, bound_2, jnp.where(pos >= bound_1, bound_1, 0))

        self.first_start = start_of(self.base)
        for r in range(self.chunks):
            start_ref[pl.ds(r * CHUNK, CHUNK)] = start_of(self.positions(r * CHUNK, CHUNK))

    def positions(self, row, size):
        rows = lax.broadcasted_iota(jnp.int32, (size, LANES), 0)
        return rows // self.group + (self.base + row // self.group)

    def low_of(self, turn, hop):
        block = (self.me ^ turn) - QUAD * hop
        low = block * self.tok
        live = (block >= 0) & (block < self.me) & (low + self.tok > self.first_start)
        return jnp.where(live, low, EMPTY)

    def scores(self, g, keys, row, size):
        first = row // self.group
        q = self.q_ref[pl.ds(first, size // self.group), pl.ds(g * self.group, self.group)]
        return lax.dot_general(
            q.reshape(size, self.dim),
            keys,
            (((1,), (1,)), ((), ())),
            preferred_element_type=jnp.float32,
        )

    def masked(self, fill, values, low, own, row, size):
        parts = []
        for h in range(0, self.tok, LANES):
            key = lax.broadcasted_iota(jnp.int32, (size, LANES), 1) + (low + h)
            seen = key >= self.start_ref[pl.ds(row, size)]
            if own:
                seen = seen & (key <= self.positions(row, size))
            parts.append(jnp.where(seen, values[:, h : h + LANES], fill))
        return jnp.concatenate(parts, axis=1)


def gained(weights, values):
    both = jnp.concatenate([values, jnp.ones_like(values)], axis=1)
    return lax.dot_general(
        weights, both, (((1,), (0,)), ((), ())), preferred_element_type=jnp.float32
    )


def stream(rows, scale, p_buf, items):
    def weigh(n):
        g, keys, _, low, own, row, _ = items[n]
        weights = jnp.exp2(rows.scores(g, keys(), row, CHUNK) * scale)
        weights = rows.masked(0.0, weights, low, own, row, CHUNK)
        p_buf[n % 2] = weights.astype(jnp.bfloat16)

    weigh(0)
    for n, (_, _, values, _, _, _, keep) in enumerate(items):
        if n + 1 < len(items):
            weigh(n + 1)
        keep(gained(p_buf[n % 2], values()))


def halves_of(ref, part, tok):
    first = 2 * tok * part
    return (lambda: ref[first : first + tok]), (lambda: ref[first + tok : first + 2 * tok])


def fetch_kernel(q_hbm, docs_ref, *refs):
    *q_outs, docs_out, sem = refs
    half, group, _ = q_outs[0].shape
    side = lax.axis_index("head")
    tokens = pl.ds(pl.multiple_of((1 - side) * half, half), half)
    copies = []
    for g, q_out in enumerate(q_outs):
        part = q_hbm.at[tokens, pl.ds(g * group, group)]
        copies.append(pltpu.make_async_copy(part, q_out, sem.at[g]))
        copies[g].start()
    docs_out[...] = docs_ref[...]
    for copy in copies:
        copy.wait()


def attend_kernel(scale, hops, groups, group, home, *refs):
    refs = list(refs)
    heads = len(groups)
    q_in = refs.pop(0)
    docs_ref = refs.pop(0)
    arrays = [[refs.pop(0) for _ in range(2 * hops + 1)] for _ in groups]
    out_ref, acc_ref, start_ref, top_ref, p_buf = refs[:5]
    side = lax.axis_index("head")
    if home:
        q_ref, piece_ref, sem = refs[5:]
        half, _, dim = q_ref.shape
        offset = pl.multiple_of(side * half, half)
        q_copy = pltpu.make_async_copy(q_in.at[pl.ds(offset, half)], q_ref, sem.at[0])
        q_copy.start()
    else:
        q_ref = q_in
        half, _, dim = q_ref.shape
        offset = pl.multiple_of((1 - side) * half, half)
    tok = 2 * half
    size = half * group
    rows = Rows(docs_ref, q_ref, group, start_ref, offset, tok)
    tables, lows = [], []
    for _, across_first in groups:
        tables.append(slot_table(rows.me, hops, across_first))
        lows.append([rows.low_of(turn, hop) for _, _, turn, hop in tables[-1]])
        lows[-1][0] = rows.me * tok
    if home:
        q_copy.wait()
    slots = range(len(tables[0]))
    chunks = size // CHUNK

    def item(n, s, row):
        keys, values = halves_of(arrays[n][tables[n][s][0]], tables[n][s][1], tok)

        def keep(gain):
            at = pl.ds(n * size + row, CHUNK)
            acc_ref[at] = gain if s == 0 else acc_ref[at] + gain

        return (n, keys, values, lows[n][s], s == 0, row, keep)

    if hops <= NEAR_HOPS:

        def run(some):
            order = [(n, s, r * CHUNK) for n in range(heads) for s in some for r in range(chunks)]
            stream(rows, scale, p_buf, [item(*at) for at in order])

        close, distant = slots[1:FAR_SLOT], slots[FAR_SLOT:]

        def held(some):
            return functools.reduce(jnp.maximum, [low[s] for low in lows for s in some]) >= 0

        every = held(close) & held(distant)
        pl.when(every)(lambda: run(slots))

        @pl.when(jnp.logical_not(every))
        def _():
            run(slots[:1])
            pl.when(held(close))(lambda: run(close))
            pl.when(held(distant))(lambda: run(distant))

    else:

        def step(r, carry):
            row = pl.multiple_of(r * CHUNK, CHUNK)
            stream(rows, scale, p_buf, [item(n, s, row) for n in range(heads) for s in slots])
            return carry

        lax.fori_loop(0, chunks, step, 0)

    total = acc_ref[:, dim:]
    bad = jnp.max(jnp.where((total < CEILING) & (total > FLOOR), 0.0, 1.0))

    @pl.when(bad > 0.0)
    def _():
        top_ref[...] = jnp.full_like(top_ref, HIDDEN)
        acc_ref[...] = jnp.zeros_like(acc_ref)
        for n in range(heads):
            for s in slots:
                keys, values = halves_of(arrays[n][tables[n][s][0]], tables[n][s][1], tok)

                def careful(i, carry, keys=keys, values=values, n=n, s=s):
                    row = pl.multiple_of(i * SMALL, SMALL)
                    at = pl.ds(pl.multiple_of(n * size + row, SMALL), SMALL)
                    scores = rows.scores(n, keys(), row, SMALL) * scale
                    scores = rows.masked(HIDDEN, scores, lows[n][s], s == 0, row, SMALL)
                    old = top_ref[at]
                    top = jnp.maximum(old, jnp.max(scores, axis=1, keepdims=True))
                    weights = jnp.exp2(scores - top[:, 0:1]).astype(jnp.bfloat16)
                    fade = jnp.exp2(old - top)
                    fade = jnp.concatenate([fade, fade], axis=1)
                    acc_ref[at] = acc_ref[at] * fade + gained(weights, values())
                    top_ref[at] = top
                    return carry

                @pl.when(lows[n][s] >= 0)
                def _(careful=careful):
                    lax.fori_loop(0, size // SMALL, careful, 0)

    span = CHUNK // group
    for n in range(heads):
        for r in range(chunks):
            gain = acc_ref[n * size + r * CHUNK : n * size + (r + 1) * CHUNK]
            done = gain[:, :dim] * pl.reciprocal(gain[:, dim:], approx=False)
            done = done.reshape(span, group, dim).astype(jnp.bfloat16)
            to = piece_ref.at[n] if home else out_ref
            to[r * span : (r + 1) * span] = done
        if home:
            start_put(piece_ref.at[n], out_ref, groups[n][0], side, sem.at[n])
    if home:
        for n in range(heads):
            start_put(piece_ref.at[n], out_ref, groups[n][0], side, sem.at[n], wait=True)


def start_put(piece, out_hbm, g, half, sem, wait=False):
    group, heads = piece.shape[1], out_hbm.shape[1]
    first = pl.multiple_of(half * (heads // 2) + g * group, group)
    copy = pltpu.make_async_copy(piece, out_hbm.at[:, pl.ds(first, group)], sem)
    if wait:
        copy.wait()
    else:
        copy.start()


def place_kernel(out_in, *refs):
    *pieces, out_ref, sem = refs
    half = 1 - lax.axis_index("head")
    for wait in (False, True):
        for g, piece in enumerate(pieces):
            start_put(piece, out_ref, g, half, sem.at[g], wait)


def on_chip(kernel, out_shape, out_specs, scratch, in_hbm, *operands, aliases=None):
    anywhere = pl.BlockSpec(memory_space=pl.ANY)
    return pl.pallas_call(
        kernel,
        out_shape=out_shape,
        in_specs=[anywhere] * len(in_hbm) + in_vmem(len(operands)),
        out_specs=out_specs,
        scratch_shapes=scratch,
        input_output_aliases=aliases or {},
    )(*in_hbm, *near(*operands))


def body(queries, key_rows, value_vectors, doc_ids):
    tok, heads_here, dim = queries.shape
    kv_heads = key_rows.shape[1]
    group = heads_here // kv_heads
    hops = hops_needed()
    scale = dim ** (-0.5) * math.log2(math.e)
    docs = doc_ids.reshape(-1, LANES)
    half = tok // 2
    output = jax.ShapeDtypeStruct((half, 2 * heads_here, dim), jnp.bfloat16)
    anywhere = pl.BlockSpec(memory_space=pl.ANY)

    own = packed(key_rows, value_vectors)
    piece = near_shape((half, group, dim), jnp.bfloat16)
    *q_away, docs = on_chip(
        fetch_kernel,
        [piece] * kv_heads + [near_shape(docs.shape, docs.dtype)],
        in_vmem(kv_heads + 1),
        [pltpu.SemaphoreType.DMA((kv_heads,))],
        [queries],
        docs,
    )

    def scratch(heads):
        rows = half * group
        return [
            pltpu.VMEM((heads * rows, 2 * dim), jnp.float32),
            pltpu.VMEM((rows, LANES), jnp.int32),
            pltpu.VMEM((heads * rows, dim), jnp.float32),
            pltpu.VMEM((2, CHUNK, tok), jnp.bfloat16),
        ]

    groups, windows, others = [], [], []
    for g in range(kv_heads):
        groups.append((g, hops == 2 and g % 2 == 1))
        windows.append(gathered(own[g], hops, groups[g][1]))
        away = on_chip(
            functools.partial(attend_kernel, scale, hops, groups[g : g + 1], group, False),
            piece,
            pl.BlockSpec(memory_space=pltpu.VMEM),
            scratch(1),
            [],
            q_away[g], docs, *windows[g],
        )
        others.append(crossed(away))
    result = on_chip(
        functools.partial(attend_kernel, scale, hops, groups, group, True),
        output,
        anywhere,
        scratch(kv_heads)
        + [
            pltpu.VMEM((half, heads_here, dim), jnp.bfloat16),
            pltpu.VMEM((kv_heads, half, group, dim), jnp.bfloat16),
            pltpu.SemaphoreType.DMA((kv_heads,)),
        ],
        [queries],
        docs, *[array for window in windows for array in window],
    )
    return on_chip(
        place_kernel, output, anywhere, [pltpu.SemaphoreType.DMA((kv_heads,))],
        [result], *others, aliases={0: 0},
    )


def solution(mesh):
    placed = (P("ctx", "head", None), P("ctx", "head", None), P("ctx", "head", None), P())

    return jax.shard_map(
        body, mesh=mesh, in_specs=placed, out_specs=P(("ctx", "head"), None, None), check_vma=False
    )
```

```python
import functools
import math

import jax
import jax.numpy as jnp
from jax import lax
from jax.experimental import pallas as pl
from jax.experimental.pallas import tpu as pltpu
from jax.sharding import PartitionSpec as P


QUAD = 4
CHUNK = 512
LANES = 128
NEAR_HOPS = 3
HIDDEN = -1e30
FAR_SLOT = 5
EMPTY = -(1 << 30)
SMALL = 64
CEILING = 2.0**100
FLOOR = 2.0**-100


def shifted(block, lowest, right_lowest=None):
    n = lax.axis_size("ctx")
    last = n // QUAD - 1
    route = []
    for i in range(n):
        plane, place = divmod(i, QUAD)
        low = lowest if right_lowest is None or place < QUAD // 2 else right_lowest
        target = plane if plane < low else low if plane == last else plane + 1
        route.append((i, target * QUAD + place))
    return lax.ppermute(block, "ctx", route)


def swapped(block, bit):
    n = lax.axis_size("ctx")
    return lax.ppermute(block, "ctx", [(i, i ^ bit) for i in range(n)])


def crossed(block):
    return lax.ppermute(block, "head", [(0, 1), (1, 0)])


def in_vmem(count):
    return [pl.BlockSpec(memory_space=pltpu.VMEM)] * count


def hops_needed():
    reach = lax.axis_size("ctx") // 2 - 1
    return -(-reach // QUAD)


def near(*arrays):
    if hops_needed() > NEAR_HOPS:
        return list(arrays)
    return [pltpu.with_memory_space_constraint(a, pltpu.VMEM) for a in arrays]


def near_shape(shape, dtype):
    if hops_needed() > NEAR_HOPS:
        return jax.ShapeDtypeStruct(shape, dtype)
    return pltpu.VMEM(shape, dtype)


def pack_kernel(k_ref, v_ref, *refs):
    *outs, k_wide, v_wide = refs
    heads = len(outs)
    tok = k_ref.shape[0] // heads
    k_wide[...] = k_ref[...].astype(jnp.float32)
    v_wide[...] = v_ref[...].astype(jnp.float32)
    for g, out in enumerate(outs):
        out[0:tok, :] = k_wide[pl.ds(g, tok, heads), :].astype(jnp.bfloat16)
        out[tok : 2 * tok, :] = v_wide[pl.ds(g, tok, heads), :].astype(jnp.bfloat16)


def packed(key_rows, value_vectors):
    tok, kv_heads, dim = key_rows.shape
    flat = (tok * kv_heads, dim)
    return pl.pallas_call(
        pack_kernel,
        out_shape=[near_shape((2 * tok, dim), jnp.bfloat16)] * kv_heads,
        in_specs=in_vmem(2),
        out_specs=in_vmem(kv_heads),
        scratch_shapes=[pltpu.VMEM(flat, jnp.float32)] * 2,
        name="pack",
    )(key_rows.reshape(flat), value_vectors.reshape(flat))


def take(out_ref, at, choices):
    for wanted, ref in choices:

        def copy(ref=ref):
            out_ref[at : at + ref.shape[0], :] = ref[...]

        if wanted is None:
            copy()
        else:
            pl.when(wanted)(copy)


def joined(first, second):
    arrays = [array for _, array in first + second]
    size, dim = arrays[0].shape

    def kernel(*refs):
        *ins, out_ref = refs
        me = lax.axis_index("ctx")
        wanted = [None if test is None else test(me) for test, _ in first + second]
        choices = list(zip(wanted, ins))
        take(out_ref, 0, choices[: len(first)])
        take(out_ref, size, choices[len(first) :])

    return pl.pallas_call(
        kernel,
        out_shape=near_shape((2 * size, dim), jnp.bfloat16),
        in_specs=in_vmem(len(arrays)),
        out_specs=pl.BlockSpec(memory_space=pltpu.VMEM),
        name="join",
    )(*near(*arrays))


def upper(me):
    return me & 1 == 1


def lower(me):
    return me & 1 == 0


def right(me):
    return me & 2 == 2


def left(me):
    return me & 2 == 0


def both(test, other):
    return lambda me: test(me) & other(me)


def chosen(test, yes, no):
    return jnp.where(test(lax.axis_index("ctx")), yes, no)


def gathered(own, g, hops, across_first):
    arrays = [own]
    line = own

    def twin(first, second):
        pair = joined(first, second)
        return [pair, swapped(pair, 1)]

    if across_first:
        beside = swapped(own, 2)
        line = shifted(own, 0)
        wide = shifted(chosen(left, beside, line), 0, 1)
        back = shifted(line, 1)
        arrays += twin([(None, line)], [(right, beside), (left, wide)])
        across = swapped(chosen(left, line, wide), 2)
        last = [(lower, own), (both(upper, right), wide), (both(upper, left), back)]
    else:
        for hop in range(1, hops):
            line = shifted(line, hop - 1)
            across = swapped(line, 2)
            arrays += twin([(None, line)], [(None, across)])
        line = shifted(line, hops - 1 if g == 0 else 0)
        across = swapped(chosen(left, own, line), 2)
        last = [(lower, own), (upper, line)]
    return arrays + [across, twin(last, [(None, across)])[1]]


def slot_table(me, hops, across_first):
    near_hop = jnp.where(right(me), 0, 1)
    far_hop = jnp.where(right(me), 1 if across_first else 0, hops)
    table = [(0, 0, 0, 0)]
    for hop in range(1, hops):
        a = 2 * hop - 1
        beside = near_hop if across_first else hop
        table += [(a, 0, 0, hop), (a, 1, 2, beside)]
        table += [(a + 1, 0, 1, hop), (a + 1, 1, 3, beside)]
    a = 2 * hops - 1
    table += [(a, 0, 2, far_hop), (a + 1, 0, 1, jnp.where(upper(me), 0, hops))]
    return table + [(a + 1, 1, 3, far_hop)]


class Rows:
    def __init__(self, docs_ref, q_ref, group, start_ref, offset, tok):
        self.q_ref, self.group, self.start_ref, self.tok = q_ref, group, start_ref, tok
        count, _, self.dim = q_ref.shape
        self.chunks = count * group // CHUNK
        self.me = lax.axis_index("ctx")
        self.base = self.me * self.tok + offset
        docs = docs_ref[...]
        bound_1 = jnp.sum((docs < 1).astype(jnp.int32))
        bound_2 = jnp.sum((docs < 2).astype(jnp.int32))

        def start_of(pos):
            return jnp.where(pos >= bound_2, bound_2, jnp.where(pos >= bound_1, bound_1, 0))

        self.first_start = start_of(self.base)
        for r in range(self.chunks):
            start_ref[pl.ds(r * CHUNK, CHUNK)] = start_of(self.positions(r * CHUNK, CHUNK))

    def positions(self, row, size):
        rows = lax.broadcasted_iota(jnp.int32, (size, LANES), 0)
        return rows // self.group + (self.base + row // self.group)

    def low_of(self, turn, hop):
        block = (self.me ^ turn) - QUAD * hop
        low = block * self.tok
        live = (block >= 0) & (block < self.me) & (low + self.tok > self.first_start)
        return jnp.where(live, low, EMPTY)

    def scores(self, g, keys, row, size):
        first = row // self.group
        q = self.q_ref[pl.ds(first, size // self.group), pl.ds(g * self.group, self.group)]
        return lax.dot_general(
            q.reshape(size, self.dim),
            keys,
            (((1,), (1,)), ((), ())),
            preferred_element_type=jnp.float32,
        )

    def masked(self, fill, values, low, own, row, size):
        parts = []
        for h in range(0, self.tok, LANES):
            key = lax.broadcasted_iota(jnp.int32, (size, LANES), 1) + (low + h)
            seen = key >= self.start_ref[pl.ds(row, size)]
            if own:
                seen = seen & (key <= self.positions(row, size))
            parts.append(jnp.where(seen, values[:, h : h + LANES], fill))
        return jnp.concatenate(parts, axis=1)


def gained(weights, values):
    both = jnp.concatenate([values, jnp.ones_like(values)], axis=1)
    return lax.dot_general(
        weights, both, (((1,), (0,)), ((), ())), preferred_element_type=jnp.float32
    )


def stream(rows, scale, p_buf, items):
    def weigh(n):
        g, keys, _, low, own, row, _ = items[n]
        weights = jnp.exp2(rows.scores(g, keys(), row, CHUNK) * scale)
        weights = rows.masked(0.0, weights, low, own, row, CHUNK)
        p_buf[n % 2] = weights.astype(jnp.bfloat16)

    weigh(0)
    for n, (_, _, values, _, _, _, keep) in enumerate(items):
        if n + 1 < len(items):
            weigh(n + 1)
        keep(gained(p_buf[n % 2], values()))


def halves_of(ref, part, tok):
    first = 2 * tok * part
    return (lambda: ref[first : first + tok]), (lambda: ref[first + tok : first + 2 * tok])


def fetch_kernel(q_hbm, docs_ref, *refs):
    *q_outs, docs_out, sem = refs
    half, group, _ = q_outs[0].shape
    side = lax.axis_index("head")
    tokens = pl.ds(pl.multiple_of((1 - side) * half, half), half)
    copies = []
    for g, q_out in enumerate(q_outs):
        part = q_hbm.at[tokens, pl.ds(g * group, group)]
        copies.append(pltpu.make_async_copy(part, q_out, sem.at[g]))
        copies[g].start()
    docs_out[...] = docs_ref[...]
    for copy in copies:
        copy.wait()


def attend_kernel(scale, hops, groups, group, home, aside, *refs):
    refs = list(refs)
    heads = len(groups)
    q_in = refs.pop(0)
    outside = [refs.pop(0) for _ in aside]
    docs_ref = refs.pop(0)
    arrays = [
        [None if (n, a) in aside else refs.pop(0) for a in range(2 * hops + 1)]
        for n in range(heads)
    ]
    out_ref, acc_ref, start_ref, top_ref, p_buf = refs[:5]
    side = lax.axis_index("head")
    loads = []
    if home:
        q_ref, piece_ref, sem = refs[5:8]
        for i, (n, a) in enumerate(aside):
            arrays[n][a] = refs[8 + i]
            loads.append(pltpu.make_async_copy(outside[i], refs[8 + i], sem.at[heads + i]))
            loads[i].start()
        half, _, dim = q_ref.shape
        offset = pl.multiple_of(side * half, half)
        q_copy = pltpu.make_async_copy(q_in.at[pl.ds(offset, half)], q_ref, sem.at[0])
        q_copy.start()
    else:
        q_ref = q_in
        half, _, dim = q_ref.shape
        offset = pl.multiple_of((1 - side) * half, half)
    tok = 2 * half
    size = half * group
    rows = Rows(docs_ref, q_ref, group, start_ref, offset, tok)
    tables, lows = [], []
    for _, across_first in groups:
        tables.append(slot_table(rows.me, hops, across_first))
        lows.append([rows.low_of(turn, hop) for _, _, turn, hop in tables[-1]])
        lows[-1][0] = rows.me * tok
    if home:
        q_copy.wait()
        for load in loads:
            load.wait()
    slots = range(len(tables[0]))
    chunks = size // CHUNK

    def item(n, s, row):
        keys, values = halves_of(arrays[n][tables[n][s][0]], tables[n][s][1], tok)

        def keep(gain):
            at = pl.ds(n * size + row, CHUNK)
            acc_ref[at] = gain if s == 0 else acc_ref[at] + gain

        return (n, keys, values, lows[n][s], s == 0, row, keep)

    if hops <= NEAR_HOPS:

        def run(some):
            order = [(n, s, r * CHUNK) for n in range(heads) for s in some for r in range(chunks)]
            stream(rows, scale, p_buf, [item(*at) for at in order])

        close, distant = slots[1:FAR_SLOT], slots[FAR_SLOT:]

        def held(some):
            return functools.reduce(jnp.maximum, [low[s] for low in lows for s in some]) >= 0

        every = held(close) & held(distant)
        pl.when(every)(lambda: run(slots))

        @pl.when(jnp.logical_not(every))
        def _():
            run(slots[:1])
            pl.when(held(close))(lambda: run(close))
            pl.when(held(distant))(lambda: run(distant))

    else:

        def step(r, carry):
            row = pl.multiple_of(r * CHUNK, CHUNK)
            stream(rows, scale, p_buf, [item(n, s, row) for n in range(heads) for s in slots])
            return carry

        lax.fori_loop(0, chunks, step, 0)

    total = acc_ref[:, dim:]
    bad = jnp.max(jnp.where((total < CEILING) & (total > FLOOR), 0.0, 1.0))

    @pl.when(bad > 0.0)
    def _():
        top_ref[...] = jnp.full_like(top_ref, HIDDEN)
        acc_ref[...] = jnp.zeros_like(acc_ref)
        for n in range(heads):
            for s in slots:
                keys, values = halves_of(arrays[n][tables[n][s][0]], tables[n][s][1], tok)

                def careful(i, carry, keys=keys, values=values, n=n, s=s):
                    row = pl.multiple_of(i * SMALL, SMALL)
                    at = pl.ds(pl.multiple_of(n * size + row, SMALL), SMALL)
                    scores = rows.scores(n, keys(), row, SMALL) * scale
                    scores = rows.masked(HIDDEN, scores, lows[n][s], s == 0, row, SMALL)
                    old = top_ref[at]
                    top = jnp.maximum(old, jnp.max(scores, axis=1, keepdims=True))
                    weights = jnp.exp2(scores - top[:, 0:1]).astype(jnp.bfloat16)
                    fade = jnp.exp2(old - top)
                    fade = jnp.concatenate([fade, fade], axis=1)
                    acc_ref[at] = acc_ref[at] * fade + gained(weights, values())
                    top_ref[at] = top
                    return carry

                @pl.when(lows[n][s] >= 0)
                def _(careful=careful):
                    lax.fori_loop(0, size // SMALL, careful, 0)

    span = CHUNK // group
    for n in range(heads):
        for r in range(chunks):
            gain = acc_ref[n * size + r * CHUNK : n * size + (r + 1) * CHUNK]
            done = gain[:, :dim] * pl.reciprocal(gain[:, dim:], approx=False)
            done = done.reshape(span, group, dim).astype(jnp.bfloat16)
            to = piece_ref.at[n] if home else out_ref
            to[r * span : (r + 1) * span] = done
        if home:
            start_put(piece_ref.at[n], out_ref, groups[n][0], side, sem.at[n])
    if home:
        for n in range(heads):
            start_put(piece_ref.at[n], out_ref, groups[n][0], side, sem.at[n], wait=True)


def start_put(piece, out_hbm, g, half, sem, wait=False):
    group, heads = piece.shape[1], out_hbm.shape[1]
    first = pl.multiple_of(half * (heads // 2) + g * group, group)
    copy = pltpu.make_async_copy(piece, out_hbm.at[:, pl.ds(first, group)], sem)
    if wait:
        copy.wait()
    else:
        copy.start()


def place_kernel(out_in, *refs):
    *pieces, out_ref, sem = refs
    half = 1 - lax.axis_index("head")
    for wait in (False, True):
        for g, piece in enumerate(pieces):
            start_put(piece, out_ref, g, half, sem.at[g], wait)


def on_chip(kernel, out_shape, out_specs, scratch, in_hbm, *operands, aliases=None):
    anywhere = pl.BlockSpec(memory_space=pl.ANY)
    return pl.pallas_call(
        kernel,
        out_shape=out_shape,
        in_specs=[anywhere] * len(in_hbm) + in_vmem(len(operands)),
        out_specs=out_specs,
        scratch_shapes=scratch,
        input_output_aliases=aliases or {},
    )(*in_hbm, *near(*operands))


def body(queries, key_rows, value_vectors, doc_ids):
    tok, heads_here, dim = queries.shape
    kv_heads = key_rows.shape[1]
    group = heads_here // kv_heads
    hops = hops_needed()
    scale = dim ** (-0.5) * math.log2(math.e)
    docs = doc_ids.reshape(-1, LANES)
    half = tok // 2
    output = jax.ShapeDtypeStruct((half, 2 * heads_here, dim), jnp.bfloat16)
    anywhere = pl.BlockSpec(memory_space=pl.ANY)

    own = packed(key_rows, value_vectors)
    piece = near_shape((half, group, dim), jnp.bfloat16)
    *q_away, docs = on_chip(
        fetch_kernel,
        [piece] * kv_heads + [near_shape(docs.shape, docs.dtype)],
        in_vmem(kv_heads + 1),
        [pltpu.SemaphoreType.DMA((kv_heads,))],
        [queries],
        docs,
    )

    def scratch(heads):
        rows = half * group
        return [
            pltpu.VMEM((heads * rows, 2 * dim), jnp.float32),
            pltpu.VMEM((rows, LANES), jnp.int32),
            pltpu.VMEM((heads * rows, dim), jnp.float32),
            pltpu.VMEM((2, CHUNK, tok), jnp.bfloat16),
        ]

    groups, windows, others = [], [], []
    for g in range(kv_heads):
        groups.append((g, False))
        windows.append(gathered(own[g], g, hops, groups[g][1]))
        away = on_chip(
            functools.partial(attend_kernel, scale, hops, groups[g : g + 1], group, False, []),
            piece,
            pl.BlockSpec(memory_space=pltpu.VMEM),
            scratch(1),
            [],
            q_away[g], docs, *windows[g],
        )
        others.append(crossed(away))
    aside = [(0, a) for a in range(2, 2 * hops + 1, 2)] if hops <= NEAR_HOPS else []
    kept = [
        array
        for n, window in enumerate(windows)
        for a, array in enumerate(window)
        if (n, a) not in aside
    ]
    result = on_chip(
        functools.partial(attend_kernel, scale, hops, groups, group, True, aside),
        output,
        anywhere,
        scratch(kv_heads)
        + [
            pltpu.VMEM((half, heads_here, dim), jnp.bfloat16),
            pltpu.VMEM((kv_heads, half, group, dim), jnp.bfloat16),
            pltpu.SemaphoreType.DMA((kv_heads + len(aside),)),
        ]
        + [pltpu.VMEM(windows[n][a].shape, jnp.bfloat16) for n, a in aside],
        [queries] + [windows[n][a] for n, a in aside],
        docs, *kept,
    )
    return on_chip(
        place_kernel, output, anywhere, [pltpu.SemaphoreType.DMA((kv_heads,))],
        [result], *others, aliases={0: 0},
    )


def solution(mesh):
    placed = (P("ctx", "head", None), P("ctx", "head", None), P("ctx", "head", None), P())

    return jax.shard_map(
        body, mesh=mesh, in_specs=placed, out_specs=P(("ctx", "head"), None, None), check_vma=False
    )
```
